512 devices in a mesh: band: 32 (over y_lo, x, core), plane: 16 (over y_hi, z).
Axes of the slice: x: 4, y: 8 (y_hi: 2, y_lo: 4; y = y_hi * 4 + y_lo), z: 8, core: 2. Of those that a mesh axis runs over, the one named last changes fastest.
Arguments:
- orbitals: bfloat16 [64, 128, 128, 128], P('band', 'plane'), may hold values from -6 to 6
- potential_slots: bfloat16 [32, 2, 128, 128, 128], P('band', None, 'plane'), may hold values from -6 to 6
- pattern_owner: int32 [4], replicated, may hold values from 0 to 31, as said below
- retained: int32 [3, 64], replicated, may hold values from 0 to 127, as said below
- band_energy: float32 [64], P('band'), may hold values from 0.5 to 8
Outputs:
- rhs: float32 [64, 4, 64, 64, 128], P('band', None, None, 'plane')
The draws below stay inside these ranges and needn't reach their ends.
Inputs may be any that keep to these rules, and one draw needn't show every extreme that they name: pattern_owner holds 4 distinct slot indices. Each row of retained holds 64 distinct frequency indices.
All inputs are finite; a program needn't handle non-finite values.
Results may differ from the reference program's by a relative error of at most 0.0003.
Values may be sent and summed in bfloat16 or wider, within the bound.
A program may use at most 64 MiB of HBM per device.

```python
import math
import jax
import jax.numpy as jnp
from jax import lax

NGRID = 128
KEEP = 64
NB = 64
NPERT = 4
N_BAND = 32


def distinct_with_ends(key, total, count):
    inner = jax.random.permutation(jax.random.fold_in(key, 3), total - 2)[:count - 2].astype(jnp.int32) + 1
    picked = jnp.concatenate([jnp.array([0, total - 1], dtype=jnp.int32), inner])
    order = jax.random.permutation(jax.random.fold_in(key, 5), count)
    return picked[order].astype(jnp.int32)


def draw_pattern_owner(key, part):
    return distinct_with_ends(jax.random.fold_in(key, 7), N_BAND, NPERT)


def draw_retained(key, part):
    chosen = [distinct_with_ends(jax.random.fold_in(key, 11 + dimension), NGRID, KEEP) for dimension in range(3)]
    return jnp.stack(chosen).astype(jnp.int32)


def level_of(key, dims, pieces, smallest, high):
    loudness, own = 1.0, jax.random.fold_in(key, 6)
    for axis_at, blocks in pieces:
        draws = jnp.exp(jax.random.uniform(jax.random.fold_in(own, axis_at), (blocks,), jnp.float32, smallest / len(pieces), high / len(pieces)))
        loudness = loudness * jnp.repeat(draws, dims[axis_at] // blocks).reshape([-1 if axis == axis_at else 1 for axis in range(len(dims))])
    return loudness


def scatter_about(own_key, shape, width, reach, shards=(), kind=jnp.bfloat16):
    values = width * jax.random.normal(own_key, shape, jnp.float32)
    if shards:
        values = values * level_of(own_key, shape, shards, -0.22, 0.18)
    return jnp.clip(values, -reach, reach).astype(kind)


def setup_inputs(seed: int = 0) -> dict:
    key_list = jax.random.split(jax.random.key(seed), 6)
    return {
        "orbitals": scatter_about(key_list[0], (NB, NGRID, NGRID, NGRID), 1.0, 6.0, ((0, 32), (1, 16))),
        "potential_slots": scatter_about(key_list[1], (N_BAND, 2, NGRID, NGRID, NGRID), 1.0, 6.0, ((0, 32), (2, 16))),
        "pattern_owner": draw_pattern_owner(jax.random.fold_in(key_list[5], 71), 0),
        "retained": draw_retained(jax.random.fold_in(key_list[5], 71), 0),
        "band_energy": jnp.clip(jnp.exp(math.log(8.0) - 2.7725887 * jax.random.uniform(key_list[4], (NB,), jnp.float32) ** level_of(key_list[4], (NB,), ((0, 32),), -0.2, 0.2)), 0.5, 8.0),
    }


kinetic_coef = 0.5 * (2.0 * math.pi / 64.0) ** 2

def freq_table(frequency, length):
    position = jnp.arange(length, dtype=jnp.int32)
    phase_index = position[:, None] * frequency[None, :].astype(jnp.int32) % length
    angles = phase_index.astype(jnp.float32) * (2.0 * math.pi / length)
    norm_factor = 1.0 / math.sqrt(length)
    return (jnp.cos(angles) * norm_factor, -jnp.sin(angles) * norm_factor)

def signed_square(frequency, length):
    signed = jnp.where(frequency < length // 2, frequency, frequency - length).astype(jnp.float32)
    return signed * signed

def complex_step(real_part, imag_part, cos_table, sin_table, einsum_form):
    highest = lax.Precision.HIGHEST
    out_real = jnp.einsum(einsum_form, real_part, cos_table, precision=highest) - jnp.einsum(einsum_form, imag_part, sin_table, precision=highest)
    out_imag = jnp.einsum(einsum_form, real_part, sin_table, precision=highest) + jnp.einsum(einsum_form, imag_part, cos_table, precision=highest)
    return (out_real, out_imag)

def reference(orbitals, potential_slots, pattern_owner, retained, band_energy):
    cos_x, sin_x = freq_table(retained[0], NGRID)
    cos_y, sin_y = freq_table(retained[1], NGRID)
    cos_z, sin_z = freq_table(retained[2], NGRID)
    kinetic = kinetic_coef * (signed_square(retained[0], NGRID)[:, None, None] + signed_square(retained[1], NGRID)[None, :, None] + signed_square(retained[2], NGRID)[None, None, :])
    potentials = jnp.take(potential_slots, pattern_owner, axis=0).astype(jnp.float32)

    def one_band(carry_in):
        orbital, energy = carry_in
        density = orbital.astype(jnp.float32)
        real_part = density[None] * potentials[:, 0]
        imag_part = density[None] * potentials[:, 1]
        real_part, imag_part = complex_step(real_part, imag_part, cos_z, sin_z, 'pxyz,zl->pxyl')
        real_part, imag_part = complex_step(real_part, imag_part, cos_y, sin_y, 'pxyl,yj->pxjl')
        real_part, imag_part = complex_step(real_part, imag_part, cos_x, sin_x, 'pxjl,xi->pijl')
        precond = 1.0 / (1.0 + kinetic / energy)
        return jnp.concatenate([real_part * precond[None], imag_part * precond[None]], axis=-1)
    return lax.map(one_band, (orbitals, band_energy))
```

```python
import functools
import math

import jax
import jax.numpy as jnp
from jax import lax
from jax.experimental import pallas as pl
from jax.experimental.pallas import tpu as pltpu
from jax.sharding import PartitionSpec as P

kinetic_coef = 0.5 * (2.0 * math.pi / 64.0) ** 2
MESH = pl.DeviceIdType.MESH
F32 = jnp.float32
BF16 = jnp.bfloat16
PAD = 72
POWER = 17.5
RANGE = 8192.0
SHIFT = 125.0 * math.log(2.0)


def make_table(frequency, length):
    position = jnp.arange(length, dtype=jnp.int32)
    phase_index = position[:, None] * frequency[None, :] % length
    angles = phase_index.astype(F32) * (2.0 * math.pi / length)
    norm_factor = 1.0 / math.sqrt(length)
    return jnp.cos(angles) * norm_factor, -jnp.sin(angles) * norm_factor


def signed_square(frequency, length):
    signed = jnp.where(frequency < length // 2, frequency, frequency - length).astype(F32)
    return signed * signed


def split(table):
    high = lax.reduce_precision(table, 8, 7)
    return high.astype(BF16), (table - high).astype(BF16)


def encode(value, inverse_scale):
    u = jnp.abs(value) * inverse_scale
    w = u + jnp.sqrt(u * u + 1.0)
    code = jnp.exp(POWER * jnp.log(w) - SHIFT)
    return jnp.where(value < 0.0, -code, code).astype(BF16)


def decode(code, scale):
    code = code.astype(F32)
    w = jnp.exp((jnp.log(jnp.abs(code)) + SHIFT) * (1.0 / POWER))
    u = (0.5 * scale) * (w - 1.0 / w)
    return jnp.where(code < 0.0, -u, u)


def parts(value):
    high = value.astype(BF16)
    return high, (value - high.astype(F32)).astype(BF16)


def dot(a, b):
    return jnp.dot(a, b, preferred_element_type=F32)


def kernel(
    owner, energy, ky2, orb, slot, wz, wy, wx, kx2, kz2, out,
    chunks, pot, cols, sent, got, scale_out, scale_in,
    a_send, a_recv, y_send, y_recv, x_send, x_recv, c_send, c_recv,
    d_send, d_recv, s_send, s_recv,
):
    band, plane = lax.axis_index("band"), lax.axis_index("plane")
    row, spot = band // 8, band % 8
    col, core = spot // 2, spot % 2
    n_pat = 4

    barrier = pltpu.get_barrier_semaphore()

    def greet_band(o, _):
        pl.semaphore_signal(barrier, 1, device_id={"band": (band + o) % 32}, device_id_type=MESH)
        return 0

    def greet_plane(o, _):
        pl.semaphore_signal(barrier, 1, device_id={"plane": (plane + o) % 16}, device_id_type=MESH)
        return 0

    lax.fori_loop(1, 32, greet_band, 0)
    lax.fori_loop(1, 16, greet_plane, 0)
    pl.semaphore_wait(barrier, 46)

    def chunk_copy(o):
        peer = (band + o) % 32
        return pltpu.make_async_remote_copy(
            src_ref=slot.at[:, peer % 8, pl.ds(pl.multiple_of(32 * (peer // 8), 32), 32), :],
            dst_ref=chunks.at[band],
            send_sem=a_send.at[o], recv_sem=a_recv.at[o],
            device_id={"band": peer}, device_id_type=MESH,
        )

    def chunk_arrival(o):
        src = (band - o + 32) % 32
        return pltpu.make_async_remote_copy(
            src_ref=chunks.at[src], dst_ref=chunks.at[src],
            send_sem=a_send.at[o], recv_sem=a_recv.at[o],
            device_id={"band": src}, device_id_type=MESH,
        )

    def loop(lo, hi, f):
        def body(o, _):
            f(o)
            return 0
        lax.fori_loop(lo, hi, body, 0)

    loop(1, 32, lambda o: chunk_copy(o).start())
    chunks[band] = slot[:, spot, pl.ds(pl.multiple_of(32 * row, 32), 32), :]
    loop(1, 32, lambda o: chunk_arrival(o).wait_recv())

    def y_copy(p, o):
        return pltpu.make_async_remote_copy(
            src_ref=pot.at[p, spot, row], dst_ref=pot.at[p, spot, row],
            send_sem=y_send.at[p, o], recv_sem=y_recv.at[p, o],
            device_id={"band": (row + o) % 4 * 8 + spot}, device_id_type=MESH,
        )

    def y_arrival(p, o):
        src = (row - o + 4) % 4
        return pltpu.make_async_remote_copy(
            src_ref=pot.at[p, spot, src], dst_ref=pot.at[p, spot, src],
            send_sem=y_send.at[p, o], recv_sem=y_recv.at[p, o],
            device_id={"band": src * 8 + spot}, device_id_type=MESH,
        )

    def x_copy(p, o):
        return pltpu.make_async_remote_copy(
            src_ref=pot.at[p, spot], dst_ref=pot.at[p, spot],
            send_sem=x_send.at[p, o], recv_sem=x_recv.at[p, o],
            device_id={"band": row * 8 + (col + o) % 4 * 2 + core}, device_id_type=MESH,
        )

    def x_arrival(p, o):
        src = (col - o + 4) % 4 * 2 + core
        return pltpu.make_async_remote_copy(
            src_ref=pot.at[p, src], dst_ref=pot.at[p, src],
            send_sem=x_send.at[p, o], recv_sem=x_recv.at[p, o],
            device_id={"band": row * 8 + src}, device_id_type=MESH,
        )

    def core_copy(p, o):
        src = (col - o + 4) % 4 * 2 + core
        return pltpu.make_async_remote_copy(
            src_ref=pot.at[p, src], dst_ref=pot.at[p, src],
            send_sem=c_send.at[p, o], recv_sem=c_recv.at[p, o],
            device_id={"band": row * 8 + col * 2 + 1 - core}, device_id_type=MESH,
        )

    def core_arrival(p, o):
        src = (col - o + 4) % 4 * 2 + 1 - core
        return pltpu.make_async_remote_copy(
            src_ref=pot.at[p, src], dst_ref=pot.at[p, src],
            send_sem=c_send.at[p, o], recv_sem=c_recv.at[p, o],
            device_id={"band": row * 8 + col * 2 + 1 - core}, device_id_type=MESH,
        )

    for p in range(n_pat):
        pot[p, spot, row] = chunks[owner[p]]
        loop(1, 4, lambda o: y_copy(p, o).start())

    def spread(p, _):
        loop(1, 4, lambda o: y_arrival(p, o).wait_recv())
        loop(1, 4, lambda o: x_copy(p, o).start())
        core_copy(p, 0).start()
        return 0

    lax.fori_loop(0, n_pat, spread, 0)

    def col_copy(p, o):
        peer = (plane + o) % 16
        return pltpu.make_async_remote_copy(
            src_ref=sent.at[p, peer], dst_ref=got.at[p, plane],
            send_sem=d_send.at[p, o], recv_sem=d_recv.at[p, o],
            device_id={"plane": peer}, device_id_type=MESH,
        )

    def col_arrival(p, o):
        src = (plane - o + 16) % 16
        return pltpu.make_async_remote_copy(
            src_ref=got.at[p, src], dst_ref=got.at[p, src],
            send_sem=d_send.at[p, o], recv_sem=d_recv.at[p, o],
            device_id={"plane": src}, device_id_type=MESH,
        )

    def scale_copy(p, o):
        return pltpu.make_async_remote_copy(
            src_ref=scale_out.at[p], dst_ref=scale_in.at[p, plane],
            send_sem=s_send.at[p, o], recv_sem=s_recv.at[p, o],
            device_id={"plane": (plane + o) % 16}, device_id_type=MESH,
        )

    def scale_arrival(p, o):
        src = (plane - o + 16) % 16
        return pltpu.make_async_remote_copy(
            src_ref=scale_in.at[p, src], dst_ref=scale_in.at[p, src],
            send_sem=s_send.at[p, o], recv_sem=s_recv.at[p, o],
            device_id={"plane": src}, device_id_type=MESH,
        )

    def pattern_step(p, _):
        def forward(o):
            x_arrival(p, o).wait_recv()
            core_copy(p, o).start()

        loop(1, 4, forward)
        loop(0, 4, lambda o: core_arrival(p, o).wait_recv())

        def pair_step(t, top):
            b, first = t // 4, t % 4 * 2
            products = []
            for h in range(2):
                orbital = orb[b, first + h].astype(F32)
                v = pot[p, first + h]
                real = v[:, 0].reshape(128, 128).astype(F32)
                imag = v[:, 1].reshape(128, 128).astype(F32)
                products.append(jnp.concatenate([orbital * real, orbital * imag], axis=1))
            high, low = parts(jnp.concatenate(products, axis=0))
            z = dot(high, wz[0]) + (dot(low, wz[0]) + dot(high, wz[1]))
            z = jnp.concatenate(
                [
                    jnp.concatenate([z[:128, :128], z[128:, :128]], axis=1),
                    jnp.concatenate([z[:128, 128:], z[128:, 128:]], axis=1),
                ],
                axis=0,
            )
            high, low = parts(z)
            both = dot(wy[...], high)
            y = both[:64] + (both[64:] + dot(wy[:64], low))
            for h in range(2):
                for j in range(4):
                    cols[pl.ds(b * 32 + j * 8 + first + h, 16, stride=PAD), :] = y[
                        j * 16 : j * 16 + 16, h * 128 : h * 128 + 128
                    ]
            return jnp.maximum(top, jnp.maximum(jnp.abs(y[:, :128]), jnp.abs(y[:, 128:])))

        top = lax.fori_loop(0, 8, pair_step, jnp.zeros((64, 128), F32))
        top = jnp.max(jnp.max(top, axis=0, keepdims=True), axis=1, keepdims=True)
        scale = jnp.maximum(top, 1e-30) * (1.0 / RANGE)
        inverse = 1.0 / scale
        scale_out[p] = jnp.broadcast_to(scale, (1, 128))
        scale_in[p, plane] = jnp.broadcast_to(scale, (1, 128))

        def encode_step(d, _):
            block = cols[pl.ds(pl.multiple_of(d * PAD, 8), 64), :]
            sent[p, d] = encode(block, inverse).reshape(8, 8, 128)
            return 0

        lax.fori_loop(0, 16, encode_step, 0)
        loop(1, 16, lambda o: scale_copy(p, o).start())
        loop(1, 16, lambda o: col_copy(p, o).start())
        got[p, plane] = sent[p, plane]
        return 0

    lax.fori_loop(0, n_pat, pattern_step, 0)

    lane = lax.broadcasted_iota(jnp.int32, (64, 128), 1)

    def finish(p, _):
        loop(1, 16, lambda o: scale_arrival(p, o).wait_recv())
        loop(1, 16, lambda o: col_arrival(p, o).wait_recv())
        scales = scale_in[p]

        def band_step(b, _):
            blocks = []
            for j in range(4):
                blocks.append(decode(got[p, :, b * 4 + j], scales).reshape(128, 128))
            high, low = parts(jnp.concatenate(blocks, axis=1))
            both = dot(wx[...], high)
            x = both[:128] + (both[128:] + dot(wx[:128], low))
            for j in range(4):
                cosine = x[:64, j * 128 : j * 128 + 128]
                sine = pltpu.roll(x[64:, j * 128 : j * 128 + 128], 64, 1)
                value = cosine + jnp.where(lane < 64, -sine, sine)
                kinetic = kinetic_coef * (kx2[...] + ky2[j] + kz2[...])
                value = value * (1.0 / (1.0 + kinetic / energy[b]))
                out[pl.ds((b * 4 + p) * 256 + j, 64, stride=4), :] = value
            return 0

        lax.fori_loop(0, 2, band_step, 0)
        return 0

    lax.fori_loop(0, n_pat, finish, 0)

    loop(1, 32, lambda o: chunk_copy(o).wait_send())

    def drain(p, _):
        loop(1, 4, lambda o: y_copy(p, o).wait_send())
        loop(1, 4, lambda o: x_copy(p, o).wait_send())
        loop(0, 4, lambda o: core_copy(p, o).wait_send())
        loop(1, 16, lambda o: scale_copy(p, o).wait_send())
        loop(1, 16, lambda o: col_copy(p, o).wait_send())
        return 0

    lax.fori_loop(0, n_pat, drain, 0)


def per_device(orbitals, potential_slots, pattern_owner, retained, band_energy):
    length = orbitals.shape[2]
    cz, sz = make_table(retained[2], length)
    wz = jnp.concatenate(
        [
            jnp.concatenate([cz, sz, -sz, cz], axis=1),
            jnp.concatenate([-sz, cz, -cz, -sz], axis=1),
        ],
        axis=0,
    )
    wz = jnp.stack(split(wz))
    cy, sy = make_table(retained[1].reshape(16, 4).T.reshape(64), length)
    wy = jnp.concatenate(split(jnp.concatenate([cy.T, sy.T], axis=1)), axis=0)
    cx, sx = make_table(retained[0], length)
    wx = jnp.concatenate(split(jnp.concatenate([cx.T, sx.T], axis=0)), axis=0)
    ky = lax.dynamic_slice_in_dim(retained[1], lax.axis_index("plane") * 4, 4)
    ky2 = signed_square(ky, length)
    kx2 = jnp.broadcast_to(signed_square(retained[0], length)[:, None], (64, 128))
    kz2 = jnp.tile(signed_square(retained[2], length), 2)[None, :]
    smem = pl.BlockSpec(memory_space=pltpu.SMEM)
    vmem = pl.BlockSpec(memory_space=pltpu.VMEM)
    dma = pltpu.SemaphoreType.DMA
    out = pl.pallas_call(
        kernel,
        out_shape=jax.ShapeDtypeStruct((2048, 128), F32),
        in_specs=[smem] * 3 + [vmem] * 7,
        out_specs=vmem,
        scratch_shapes=[
            pltpu.VMEM((32, 2, 32, 128), BF16),
            pltpu.VMEM((4, 8, 4, 2, 32, 128), BF16),
            pltpu.VMEM((16 * PAD, 128), F32),
            pltpu.VMEM((4, 16, 8, 8, 128), BF16),
            pltpu.VMEM((4, 16, 8, 8, 128), BF16),
            pltpu.VMEM((4, 1, 128), F32),
            pltpu.VMEM((4, 16, 1, 128), F32),
            dma((32,)), dma((32,)),
            dma((4, 4)), dma((4, 4)), dma((4, 4)), dma((4, 4)), dma((4, 4)), dma((4, 4)),
            dma((4, 16)), dma((4, 16)), dma((4, 16)), dma((4, 16)),
        ],
        compiler_params=pltpu.CompilerParams(
            collective_id=0, has_side_effects=True, vmem_limit_bytes=48 * 1024 * 1024
        ),
    )(
        pattern_owner, band_energy, ky2, orbitals, potential_slots[0],
        wz, wy, wx, kx2, kz2,
    )
    return out.reshape(2, 4, 64, 4, 128)


def solution(mesh):
    in_specs = (
        P("band", "plane", None, None),
        P("band", None, "plane", None, None),
        P(),
        P(),
        P("band"),
    )
    out_specs = P("band", None, None, "plane", None)
    return jax.shard_map(
        per_device, mesh=mesh, in_specs=in_specs, out_specs=out_specs, check_vma=False
    )
```

```python
import functools
import math

import jax
import jax.numpy as jnp
from jax import lax
from jax.experimental import pallas as pl
from jax.experimental.pallas import tpu as pltpu
from jax.sharding import PartitionSpec as P

kinetic_coef = 0.5 * (2.0 * math.pi / 64.0) ** 2
MESH = pl.DeviceIdType.MESH
F32 = jnp.float32
BF16 = jnp.bfloat16
PAD = 72
POWER = 17.5
RANGE = 8192.0
SHIFT = 125.0 * math.log(2.0)


def table(phase):
    angles = (phase & 127).astype(F32) * (2.0 * math.pi / 128)
    return jnp.cos(angles) * (1.0 / math.sqrt(128))


def signed_square(frequency):
    signed = jnp.where(frequency < 64, frequency, frequency - 128).astype(F32)
    return signed * signed


def iota(shape, dimension):
    return lax.broadcasted_iota(jnp.int32, shape, dimension)


def encode(value, inverse_scale):
    u = jnp.abs(value) * inverse_scale
    w = u + jnp.sqrt(u * u + 1.0)
    code = jnp.exp(POWER * jnp.log(w) - SHIFT)
    return jnp.where(value < 0.0, -code, code).astype(BF16)


def decode(code, scale):
    code = code.astype(F32)
    w = jnp.exp((jnp.log(jnp.abs(code)) + SHIFT) * (1.0 / POWER))
    u = (0.5 * scale) * (w - 1.0 / w)
    return jnp.where(code < 0.0, -u, u)


def parts(value):
    high = value.astype(BF16)
    return high, (value - high.astype(F32)).astype(BF16)


def dot(a, b):
    return jnp.dot(a, b, preferred_element_type=F32)


def loop(low, high, step):
    def body(o, _):
        step(o)
        return 0

    lax.fori_loop(low, high, body, 0)


def kernel(
    owner, energy, kept_scalar, kept, orb_hbm, slot_hbm, out,
    orb, slot, wz, wy, wx, precond,
    chunks, picked, pot, cols, sent, got, scale_out, scale_in, plain,
    load, a_send, a_recv, b_send, b_recv, y_send, y_recv, x_send, x_recv, c_send, c_recv,
    d_send, d_recv, s_send, s_recv,
):
    band, plane = lax.axis_index("band"), lax.axis_index("plane")
    row, spot = band // 8, band % 8
    half, upper = row // 2, row % 2
    member = band % 16
    col, core = spot // 2, spot % 2

    def remote(src, dst, send_sem, recv_sem, **to):
        return pltpu.make_async_remote_copy(
            src_ref=src, dst_ref=dst, send_sem=send_sem, recv_sem=recv_sem,
            device_id=to, device_id_type=MESH,
        )

    load_slot = pltpu.make_async_copy(slot_hbm.at[0], slot, load.at[0])
    load_orb = pltpu.make_async_copy(orb_hbm, orb, load.at[1])
    load_slot.start()
    load_orb.start()

    barrier = pltpu.get_barrier_semaphore()

    def greet(**to):
        pl.semaphore_signal(barrier, 1, device_id=to, device_id_type=MESH)

    loop(1, 16, lambda o: greet(band=half * 16 + (member + o) % 16))
    greet(band=(band + 16) % 32)
    loop(1, 16, lambda o: greet(plane=(plane + o) % 16))
    pl.semaphore_wait(barrier, 31)
    load_slot.wait()

    def chunk_of(h, to_spot, to_upper):
        rows = pl.multiple_of(to_spot % 4 * 32 + to_upper * 16, 16)
        return slot.at[:, 2 * h + to_spot // 4, pl.ds(rows, 16), :]

    def chunk_copy(h, o):
        peer = (member + o) % 16
        return remote(
            chunk_of(h, peer % 8, peer // 8), chunks.at[h, member],
            a_send.at[h, o], a_recv.at[h, o], band=half * 16 + peer,
        )

    def chunk_arrival(h, o):
        src = (member - o + 16) % 16
        return remote(
            chunks.at[h, src], chunks.at[h, src],
            a_send.at[h, o], a_recv.at[h, o], band=half * 16 + src,
        )

    def half_copy(h):
        return remote(
            picked.at[h, 0], picked.at[h, 1], b_send.at[h], b_recv.at[h], band=(band + 16) % 32
        )

    def half_arrival(h):
        return remote(
            picked.at[h, 1], picked.at[h, 1], b_send.at[h], b_recv.at[h], band=(band + 16) % 32
        )

    def neighbour():
        return half * 16 + (1 - upper) * 8 + spot

    def y_copy(h):
        return remote(
            pot.at[h, spot, upper], pot.at[h, spot, upper],
            y_send.at[h], y_recv.at[h], band=neighbour(),
        )

    def y_arrival(h):
        return remote(
            pot.at[h, spot, 1 - upper], pot.at[h, spot, 1 - upper],
            y_send.at[h], y_recv.at[h], band=neighbour(),
        )

    def x_copy(h, o):
        return remote(
            pot.at[h, spot], pot.at[h, spot], x_send.at[h, o], x_recv.at[h, o],
            band=row * 8 + (col + o) % 4 * 2 + core,
        )

    def x_arrival(h, o):
        src = (col - o + 4) % 4 * 2 + core
        return remote(
            pot.at[h, src], pot.at[h, src], x_send.at[h, o], x_recv.at[h, o], band=row * 8 + src
        )

    def core_copy(h, o):
        src = (col - o + 4) % 4 * 2 + core
        return remote(
            pot.at[h, src], pot.at[h, src], c_send.at[h, o], c_recv.at[h, o],
            band=row * 8 + col * 2 + 1 - core,
        )

    def core_arrival(h, o):
        src = (col - o + 4) % 4 * 2 + 1 - core
        return remote(
            pot.at[h, src], pot.at[h, src], c_send.at[h, o], c_recv.at[h, o],
            band=row * 8 + col * 2 + 1 - core,
        )

    def col_copy(h, o):
        peer = (plane + o) % 16
        return remote(
            sent.at[h, peer], got.at[h, plane], d_send.at[h, o], d_recv.at[h, o], plane=peer
        )

    def col_arrival(h, o):
        src = (plane - o + 16) % 16
        return remote(
            got.at[h, src], got.at[h, src], d_send.at[h, o], d_recv.at[h, o], plane=src
        )

    def scale_copy(h, o):
        return remote(
            scale_out.at[h], scale_in.at[h, plane], s_send.at[h, o], s_recv.at[h, o],
            plane=(plane + o) % 16,
        )

    def scale_arrival(h, o):
        src = (plane - o + 16) % 16
        return remote(
            scale_in.at[h, src], scale_in.at[h, src], s_send.at[h, o], s_recv.at[h, o], plane=src
        )

    def send_chunks(h):
        loop(1, 16, lambda o: chunk_copy(h, o).start())
        rows = pl.multiple_of(spot % 4 * 32 + upper * 16, 16)
        chunks[h, member] = slot[:, 2 * h + spot // 4, pl.ds(rows, 16), :]

    send_chunks(0)
    send_chunks(1)

    lane4 = iota((1, 256), 1) // 64
    shift_top = jnp.where(lane4 == 1, 32, jnp.where(lane4 == 2, 96, 0))
    shift_low = jnp.where(lane4 == 1, 0, jnp.where(lane4 == 2, 64, 96))
    position = iota((256, 256), 0)
    freq_z = jnp.concatenate([kept[2:3, :]] * 4, axis=1)
    phase = (position & 127) * freq_z + jnp.where(position < 128, shift_top, shift_low)
    high, low = parts(table(phase))
    wz[0] = high
    wz[1] = low
    quarter = jnp.where(iota((1, 128), 1) < 64, 0, 32)
    position = iota((128, 128), 0)
    freq_y = jnp.concatenate([kept[1:2, :]] * 2, axis=1)
    cols[0:128, :] = table(position * freq_y + quarter).T
    for j in range(4):
        for k in range(2):
            high, low = parts(cols[pl.ds(k * 64 + j, 16, stride=4), :])
            wy[j * 16 : j * 16 + 16, k * 128 : k * 128 + 128] = high
            wy[64 + j * 16 : 80 + j * 16, k * 128 : k * 128 + 128] = low
    freq_x = jnp.concatenate([kept[0:1, :]] * 2, axis=1)
    position = position // 2 % 16 * 8 + position // 32 * 2 + position % 2
    high, low = parts(table(position * freq_x + quarter).T)
    wx[:128] = high
    wx[128:] = low
    kx2 = jnp.broadcast_to(signed_square(freq_x), (128, 128)).T[:64]
    kz2 = signed_square(jnp.concatenate([kept[2:3, :]] * 2, axis=1))
    for j in range(4):
        ky2 = signed_square(kept_scalar[1, plane * 4 + j])
        kinetic = kinetic_coef * (kx2 + ky2 + kz2)
        for b in range(2):
            precond[b * 4 + j] = 1.0 / (1.0 + kinetic / energy[b])
    load_orb.wait()

    def pick(h):
        loop(1, 16, lambda o: chunk_arrival(h, o).wait_recv())
        wanted = [owner[p] % 16 for p in range(4)]
        found = [chunks[h, 0]] * 4
        for m in range(1, 16):
            chunk = chunks[h, m]
            found = [jnp.where(wanted[p] == m, chunk, found[p]) for p in range(4)]
        for p in range(4):
            picked[h, 0, p] = found[p]
        half_copy(h).start()

    def settle(h):
        half_arrival(h).wait_recv()
        for p in range(4):
            inside = owner[p] // 16 == half
            pot[h, spot, upper, p] = jnp.where(inside, picked[h, 0, p], picked[h, 1, p])
        y_copy(h).start()

    def spread(h):
        y_arrival(h).wait_recv()
        loop(1, 4, lambda o: x_copy(h, o).start())
        core_copy(h, 0).start()

    def forward(h):
        def step(o):
            x_arrival(h, o).wait_recv()
            core_copy(h, o).start()

        loop(1, 4, step)

    def transform(h):
        loop(0, 4, lambda o: core_arrival(h, o).wait_recv())

        def band_step(b, top):
            products = []
            for p in range(4):
                for k in range(2):
                    orbital = orb[b, 2 * h + k].astype(F32)
                    real = pot[h, k * 4 : k * 4 + 4, :, p, 0].reshape(128, 128).astype(F32)
                    imag = pot[h, k * 4 : k * 4 + 4, :, p, 1].reshape(128, 128).astype(F32)
                    products.append(jnp.concatenate([orbital * real, orbital * imag], axis=1))
            high, low = parts(jnp.concatenate(products, axis=0))
            z = dot(high, wz[0]) + (dot(low, wz[0]) + dot(high, wz[1]))
            for p in range(4):
                even = z[p * 256 : p * 256 + 128]
                odd = z[p * 256 + 128 : p * 256 + 256]
                pair = jnp.concatenate(
                    [
                        jnp.concatenate([even[:, :128], odd[:, :128]], axis=1),
                        jnp.concatenate([even[:, 128:], odd[:, 128:]], axis=1),
                    ],
                    axis=0,
                )
                high, low = parts(pair)
                both = dot(wy[...], high)
                y = both[:64] + (both[64:] + dot(wy[:64], low))
                for k in range(2):
                    for j in range(4):
                        cols[pl.ds(b * 32 + p * 8 + k * 4 + j, 16, stride=PAD), :] = y[
                            j * 16 : j * 16 + 16, k * 128 : k * 128 + 128
                        ]
                top = jnp.maximum(top, jnp.maximum(jnp.abs(y[:, :128]), jnp.abs(y[:, 128:])))
            return top

        top = lax.fori_loop(0, 2, band_step, jnp.zeros((64, 128), F32))
        top = jnp.max(jnp.max(top, axis=0, keepdims=True), axis=1, keepdims=True)
        scale = jnp.maximum(top, 1e-30) * (1.0 / RANGE)
        inverse = 1.0 / scale
        scale_out[h] = jnp.broadcast_to(scale, (1, 128))
        scale_in[h, plane] = jnp.broadcast_to(scale, (1, 128))

        def encode_step(d, _):
            block = cols[pl.ds(pl.multiple_of(d * PAD, 8), 64), :]
            sent[h, d] = encode(block, inverse).reshape(8, 8, 128)
            return 0

        lax.fori_loop(0, 16, encode_step, 0, unroll=4)
        loop(1, 16, lambda o: scale_copy(h, o).start())
        loop(1, 16, lambda o: col_copy(h, o).start())
        got[h, plane] = sent[h, plane]

    def stage(t, _):
        @pl.when(t >= 4)
        def _():
            transform(t - 4)

        @pl.when((t >= 3) & (t < 7))
        def _():
            forward(t - 3)

        @pl.when((t >= 2) & (t < 6))
        def _():
            spread(t - 2)

        @pl.when((t >= 1) & (t < 5))
        def _():
            settle(t - 1)

        @pl.when(t < 4)
        def _():
            pick(t)

        @pl.when(t < 2)
        def _():
            send_chunks(t + 2)

        return 0

    lax.fori_loop(0, 8, stage, 0)

    def receive(h, _):
        loop(1, 16, lambda o: scale_arrival(h, o).wait_recv())
        loop(1, 16, lambda o: col_arrival(h, o).wait_recv())
        scales = scale_in[h]
        for n in range(8):
            rows = pl.multiple_of(n * 512 + h * 128, 128)
            plain[pl.ds(rows, 128), :] = decode(got[h, :, n], scales).reshape(128, 128)
        return 0

    lax.fori_loop(0, 4, receive, 0)

    lane = iota((64, 128), 1)

    def finish(n, _):
        blocks = [plain[pl.ds(n * 512 + j, 128, stride=4), :] for j in range(4)]
        high, low = parts(jnp.concatenate(blocks, axis=1))
        both = dot(wx[...], high)
        x = both[:128] + (both[128:] + dot(wx[:128], low))
        for j in range(4):
            cosine = x[:64, j * 128 : j * 128 + 128]
            sine = pltpu.roll(x[64:, j * 128 : j * 128 + 128], 64, 1)
            value = cosine + jnp.where(lane < 64, -sine, sine)
            out[pl.ds(n * 256 + j, 64, stride=4), :] = value * precond[n // 4 * 4 + j]
        return 0

    lax.fori_loop(0, 8, finish, 0, unroll=2)

    def drain(h, _):
        loop(1, 16, lambda o: chunk_copy(h, o).wait_send())
        half_copy(h).wait_send()
        y_copy(h).wait_send()
        loop(1, 4, lambda o: x_copy(h, o).wait_send())
        loop(0, 4, lambda o: core_copy(h, o).wait_send())
        loop(1, 16, lambda o: scale_copy(h, o).wait_send())
        loop(1, 16, lambda o: col_copy(h, o).wait_send())
        return 0

    lax.fori_loop(0, 4, drain, 0)


def per_device(orbitals, potential_slots, pattern_owner, retained, band_energy):
    smem = pl.BlockSpec(memory_space=pltpu.SMEM)
    vmem = pl.BlockSpec(memory_space=pltpu.VMEM)
    dma = pltpu.SemaphoreType.DMA
    out = pl.pallas_call(
        kernel,
        out_shape=jax.ShapeDtypeStruct((2048, 128), F32),
        in_specs=[smem] * 3 + [vmem] + [pl.BlockSpec(memory_space=pl.ANY)] * 2,
        out_specs=vmem,
        scratch_shapes=[
            pltpu.VMEM((2, 8, 128, 128), BF16),
            pltpu.VMEM((2, 8, 128, 128), BF16),
            pltpu.VMEM((2, 256, 256), BF16),
            pltpu.VMEM((128, 256), BF16),
            pltpu.VMEM((256, 128), BF16),
            pltpu.VMEM((8, 64, 128), F32),
            pltpu.VMEM((4, 16, 2, 16, 128), BF16),
            pltpu.VMEM((4, 2, 4, 2, 16, 128), BF16),
            pltpu.VMEM((4, 8, 2, 4, 2, 16, 128), BF16),
            pltpu.VMEM((16 * PAD, 128), F32),
            pltpu.VMEM((4, 16, 8, 8, 128), BF16),
            pltpu.VMEM((4, 16, 8, 8, 128), BF16),
            pltpu.VMEM((4, 1, 128), F32),
            pltpu.VMEM((4, 16, 1, 128), F32),
            pltpu.VMEM((4096, 128), F32),
            dma((2,)), dma((4, 16)), dma((4, 16)), dma((4,)), dma((4,)), dma((4,)), dma((4,)),
            dma((4, 4)), dma((4, 4)), dma((4, 4)), dma((4, 4)),
            dma((4, 16)), dma((4, 16)), dma((4, 16)), dma((4, 16)),
        ],
        compiler_params=pltpu.CompilerParams(
            collective_id=0, has_side_effects=True, vmem_limit_bytes=60 * 1024 * 1024
        ),
    )(pattern_owner, band_energy, retained, retained, orbitals, potential_slots)
    return out.reshape(2, 4, 64, 4, 128)


def solution(mesh):
    in_specs = (
        P("band", "plane", None, None),
        P("band", None, "plane", None, None),
        P(),
        P(),
        P("band"),
    )
    out_specs = P("band", None, None, "plane", None)
    return jax.shard_map(
        per_device, mesh=mesh, in_specs=in_specs, out_specs=out_specs, check_vma=False
    )
```

```python
import functools
import math

import jax
import jax.numpy as jnp
from jax import lax
from jax.experimental import pallas as pl
from jax.experimental.pallas import tpu as pltpu
from jax.sharding import PartitionSpec as P

kinetic_coef = 0.5 * (2.0 * math.pi / 64.0) ** 2
MESH = pl.DeviceIdType.MESH
F32 = jnp.float32
BF16 = jnp.bfloat16
PAD = 72
UNR = True
POWER = 17.5
RANGE = 8192.0
SHIFT = 125.0 * math.log(2.0)


def table(phase):
    half = (((phase + 64) & 127) - 64).astype(F32) * (math.pi / 128)
    square = half * half
    series = jnp.full_like(half, 1.0 / math.factorial(13))
    for n in (11, 9, 7, 5, 3, 1):
        series = (1.0 if n % 4 == 1 else -1.0) / math.factorial(n) + series * square
    sine = half * series
    return (1.0 - 2.0 * sine * sine) * (1.0 / math.sqrt(128))


def signed_square(frequency):
    signed = jnp.where(frequency < 64, frequency, frequency - 128).astype(F32)
    return signed * signed


def iota(shape, dimension):
    return lax.broadcasted_iota(jnp.int32, shape, dimension)


def encode(value, inverse_scale):
    u = jnp.abs(value) * inverse_scale
    w = u + jnp.sqrt(u * u + 1.0)
    code = jnp.exp(POWER * jnp.log(w) - SHIFT)
    return jnp.where(value < 0.0, -code, code).astype(BF16)


def decode(code, scale):
    code = code.astype(F32)
    w = jnp.exp((jnp.log(jnp.abs(code)) + SHIFT) * (1.0 / POWER))
    u = (0.5 * scale) * (w - 1.0 / w)
    return jnp.where(code < 0.0, -u, u)


def parts(value):
    high = value.astype(BF16)
    return high, (value - high.astype(F32)).astype(BF16)


def dot(a, b):
    return jnp.dot(a, b, preferred_element_type=F32)


def loop(low, high, step):
    def body(o, _):
        step(o)
        return 0

    lax.fori_loop(low, high, body, 0, unroll=UNR)


def kernel(
    owner, energy, kept_scalar, kept, orb_hbm, slot_hbm, out,
    orb, slot, wz, wy, wx, precond,
    chunks, picked, pot, cols, sent, got, scale_out, scale_in, plain, partial,
    load, a_send, a_recv, b_send, b_recv, y_send, y_recv, x_send, x_recv, c_send, c_recv,
    d_send, d_recv, s_send, s_recv,
):
    band, plane = lax.axis_index("band"), lax.axis_index("plane")
    row, spot = band // 8, band % 8
    half, upper = row // 2, row % 2
    member = band % 16
    col, core = spot // 2, spot % 2

    def remote(src, dst, send_sem, recv_sem, **to):
        return pltpu.make_async_remote_copy(
            src_ref=src, dst_ref=dst, send_sem=send_sem, recv_sem=recv_sem,
            device_id=to, device_id_type=MESH,
        )

    load_slot = pltpu.make_async_copy(slot_hbm.at[0], slot, load.at[0])
    load_orb = pltpu.make_async_copy(orb_hbm, orb, load.at[1])
    load_slot.start()
    load_orb.start()

    barrier = pltpu.get_barrier_semaphore()

    def greet(**to):
        pl.semaphore_signal(barrier, 1, device_id=to, device_id_type=MESH)

    loop(1, 16, lambda o: greet(band=half * 16 + (member + o) % 16))
    greet(band=(band + 16) % 32)
    loop(1, 16, lambda o: greet(plane=(plane + o) % 16))
    pl.semaphore_wait(barrier, 31)
    load_slot.wait()

    def chunk_of(h, to_spot, to_upper):
        rows = pl.multiple_of(to_spot % 4 * 32 + to_upper * 16, 16)
        return slot.at[:, 2 * h + to_spot // 4, pl.ds(rows, 16), :]

    def chunk_copy(h, o):
        peer = (member + o) % 16
        return remote(
            chunk_of(h, peer % 8, peer // 8), chunks.at[h, member],
            a_send.at[h, o], a_recv.at[h, o], band=half * 16 + peer,
        )

    def chunk_arrival(h, o):
        src = (member - o + 16) % 16
        return remote(
            chunks.at[h, src], chunks.at[h, src],
            a_send.at[h, o], a_recv.at[h, o], band=half * 16 + src,
        )

    def half_copy(h):
        return remote(
            picked.at[h, 0], picked.at[h, 1], b_send.at[h], b_recv.at[h], band=(band + 16) % 32
        )

    def half_arrival(h):
        return remote(
            picked.at[h, 1], picked.at[h, 1], b_send.at[h], b_recv.at[h], band=(band + 16) % 32
        )

    def neighbour():
        return half * 16 + (1 - upper) * 8 + spot

    def y_copy(h):
        return remote(
            pot.at[h, spot, upper], pot.at[h, spot, upper],
            y_send.at[h], y_recv.at[h], band=neighbour(),
        )

    def y_arrival(h):
        return remote(
            pot.at[h, spot, 1 - upper], pot.at[h, spot, 1 - upper],
            y_send.at[h], y_recv.at[h], band=neighbour(),
        )

    def x_copy(h, o):
        return remote(
            pot.at[h, spot], pot.at[h, spot], x_send.at[h, o], x_recv.at[h, o],
            band=row * 8 + (col + o) % 4 * 2 + core,
        )

    def x_arrival(h, o):
        src = (col - o + 4) % 4 * 2 + core
        return remote(
            pot.at[h, src], pot.at[h, src], x_send.at[h, o], x_recv.at[h, o], band=row * 8 + src
        )

    def core_copy(h, o):
        src = (col - o + 4) % 4 * 2 + core
        return remote(
            pot.at[h, src], pot.at[h, src], c_send.at[h, o], c_recv.at[h, o],
            band=row * 8 + col * 2 + 1 - core,
        )

    def core_arrival(h, o):
        src = (col - o + 4) % 4 * 2 + 1 - core
        return remote(
            pot.at[h, src], pot.at[h, src], c_send.at[h, o], c_recv.at[h, o],
            band=row * 8 + col * 2 + 1 - core,
        )

    def col_copy(h, o):
        peer = (plane + o) % 16
        return remote(
            sent.at[h, peer], got.at[h, plane], d_send.at[h, o], d_recv.at[h, o], plane=peer
        )

    def col_arrival(h, o):
        src = (plane - o + 16) % 16
        return remote(
            got.at[h, src], got.at[h, src], d_send.at[h, o], d_recv.at[h, o], plane=src
        )

    def scale_copy(h, o):
        return remote(
            scale_out.at[h], scale_in.at[h, plane], s_send.at[h, o], s_recv.at[h, o],
            plane=(plane + o) % 16,
        )

    def scale_arrival(h, o):
        src = (plane - o + 16) % 16
        return remote(
            scale_in.at[h, src], scale_in.at[h, src], s_send.at[h, o], s_recv.at[h, o], plane=src
        )

    def send_chunks(h):
        loop(1, 16, lambda o: chunk_copy(h, o).start())
        rows = pl.multiple_of(spot % 4 * 32 + upper * 16, 16)
        chunks[h, member] = slot[:, 2 * h + spot // 4, pl.ds(rows, 16), :]

    send_chunks(0)
    send_chunks(1)

    lane4 = iota((1, 256), 1) // 64
    shift_top = jnp.where(lane4 == 1, 32, jnp.where(lane4 == 2, 96, 0))
    shift_low = jnp.where(lane4 == 1, 0, jnp.where(lane4 == 2, 64, 96))
    position = iota((256, 256), 0)
    freq_z = jnp.concatenate([kept[2:3, :]] * 4, axis=1)
    phase = (position & 127) * freq_z + jnp.where(position < 128, shift_top, shift_low)
    high, low = parts(table(phase))
    wz[0] = high
    wz[1] = low
    quarter = jnp.where(iota((1, 128), 1) < 64, 0, 32)
    position = iota((128, 128), 0)
    freq_y = jnp.concatenate([kept[1:2, :]] * 2, axis=1)
    cols[0:128, :] = table(position * freq_y + quarter).T
    for j in range(4):
        for k in range(2):
            high, low = parts(cols[pl.ds(k * 64 + j, 16, stride=4), :])
            wy[j * 16 : j * 16 + 16, k * 128 : k * 128 + 128] = high
            wy[64 + j * 16 : 80 + j * 16, k * 128 : k * 128 + 128] = low
    load_orb.wait()

    def pick(h):
        loop(1, 16, lambda o: chunk_arrival(h, o).wait_recv())
        wanted = [owner[p] % 16 for p in range(4)]
        found = [chunks[h, 0]] * 4
        for m in range(1, 16):
            chunk = chunks[h, m]
            found = [jnp.where(wanted[p] == m, chunk, found[p]) for p in range(4)]
        for p in range(4):
            picked[h, 0, p] = found[p]
        half_copy(h).start()

    def settle(h):
        half_arrival(h).wait_recv()
        for p in range(4):
            inside = owner[p] // 16 == half
            pot[h, spot, upper, p] = jnp.where(inside, picked[h, 0, p], picked[h, 1, p])
        y_copy(h).start()

    def spread(h):
        y_arrival(h).wait_recv()
        loop(1, 4, lambda o: x_copy(h, o).start())
        core_copy(h, 0).start()

    def forward(h):
        def step(o):
            x_arrival(h, o).wait_recv()
            core_copy(h, o).start()

        loop(1, 4, step)

    def transform(h):
        loop(0, 4, lambda o: core_arrival(h, o).wait_recv())

        def band_step(b, top):
            products = []
            for p in range(4):
                for k in range(2):
                    orbital = orb[b, 2 * h + k].astype(F32)
                    real = pot[h, k * 4 : k * 4 + 4, :, p, 0].reshape(128, 128).astype(F32)
                    imag = pot[h, k * 4 : k * 4 + 4, :, p, 1].reshape(128, 128).astype(F32)
                    products.append(jnp.concatenate([orbital * real, orbital * imag], axis=1))
            high, low = parts(jnp.concatenate(products, axis=0))
            z = dot(high, wz[0]) + (dot(low, wz[0]) + dot(high, wz[1]))
            for p in range(4):
                even = z[p * 256 : p * 256 + 128]
                odd = z[p * 256 + 128 : p * 256 + 256]
                pair = jnp.concatenate(
                    [
                        jnp.concatenate([even[:, :128], odd[:, :128]], axis=1),
                        jnp.concatenate([even[:, 128:], odd[:, 128:]], axis=1),
                    ],
                    axis=0,
                )
                high, low = parts(pair)
                both = dot(wy[...], high)
                y = both[:64] + (both[64:] + dot(wy[:64], low))
                for k in range(2):
                    for j in range(4):
                        cols[pl.ds(b * 32 + p * 8 + k * 4 + j, 16, stride=PAD), :] = y[
                            j * 16 : j * 16 + 16, k * 128 : k * 128 + 128
                        ]
                top = jnp.maximum(top, jnp.maximum(jnp.abs(y[:, :128]), jnp.abs(y[:, 128:])))
            return top

        top = lax.fori_loop(0, 2, band_step, jnp.zeros((64, 128), F32))
        top = jnp.max(jnp.max(top, axis=0, keepdims=True), axis=1, keepdims=True)
        scale = jnp.maximum(top, 1e-30) * (1.0 / RANGE)
        inverse = 1.0 / scale
        scale_out[h] = jnp.broadcast_to(scale, (1, 128))
        scale_in[h, plane] = jnp.broadcast_to(scale, (1, 128))

        def encode_step(d, _):
            block = cols[pl.ds(pl.multiple_of(d * PAD, 8), 64), :]
            sent[h, d] = encode(block, inverse).reshape(8, 8, 128)
            return 0

        lax.fori_loop(0, 16, encode_step, 0, unroll=4)
        loop(1, 16, lambda o: scale_copy(h, o).start())
        loop(1, 16, lambda o: col_copy(h, o).start())
        got[h, plane] = sent[h, plane]

    def stage(t, _):
        @pl.when(t >= 4)
        def _():
            transform(t - 4)

        @pl.when((t >= 3) & (t < 7))
        def _():
            forward(t - 3)

        @pl.when((t >= 2) & (t < 6))
        def _():
            spread(t - 2)

        @pl.when((t >= 1) & (t < 5))
        def _():
            settle(t - 1)

        @pl.when(t < 4)
        def _():
            pick(t)

        @pl.when(t < 2)
        def _():
            send_chunks(t + 2)

        return 0

    lax.fori_loop(0, 8, stage, 0)

    freq_x = jnp.concatenate([kept[0:1, :]] * 2, axis=1)
    position = position // 2 % 16 * 8 + position // 32 * 2 + position % 2
    high, low = parts(table(position * freq_x + quarter).T)
    wx[:128] = high
    wx[128:] = low
    kx2 = jnp.broadcast_to(signed_square(freq_x), (128, 128)).T[:64]
    kz2 = signed_square(jnp.concatenate([kept[2:3, :]] * 2, axis=1))
    for j in range(4):
        ky2 = signed_square(kept_scalar[1, plane * 4 + j])
        kinetic = kinetic_coef * (kx2 + ky2 + kz2)
        for b in range(2):
            precond[b * 4 + j] = 1.0 / (1.0 + kinetic / energy[b])

    def receive(h):
        loop(1, 16, lambda o: scale_arrival(h, o).wait_recv())
        loop(1, 16, lambda o: col_arrival(h, o).wait_recv())
        scales = scale_in[h]
        for n in range(8):
            rows = pl.multiple_of(n * 512 + h * 128, 128)
            plain[pl.ds(rows, 128), :] = decode(got[h, :, n], scales).reshape(128, 128)

    def x_sum(n, first, count):
        blocks = [plain[pl.ds(n * 512 + first * 128 + j, 32 * count, stride=4), :] for j in range(4)]
        high, low = parts(jnp.concatenate(blocks, axis=1))
        keys = slice(first * 32, (first + count) * 32)
        both = dot(wx[:, keys], high)
        return both[:128] + (both[128:] + dot(wx[:128, keys], low))

    lane = iota((64, 128), 1)

    def begin(n, _):
        partial[n] = x_sum(n, 0, 3)
        return 0

    def finish(n, _):
        x = partial[n] + x_sum(n, 3, 1)
        for j in range(4):
            cosine = x[:64, j * 128 : j * 128 + 128]
            sine = pltpu.roll(x[64:, j * 128 : j * 128 + 128], 64, 1)
            value = cosine + jnp.where(lane < 64, -sine, sine)
            out[pl.ds(n * 256 + j, 64, stride=4), :] = value * precond[n // 4 * 4 + j]
        return 0

    lax.fori_loop(0, 3, lambda h, c: (receive(h), c)[1], 0)
    lax.fori_loop(0, 8, begin, 0, unroll=2)
    receive(3)
    lax.fori_loop(0, 8, finish, 0, unroll=2)

    def drain(h, _):
        loop(1, 16, lambda o: chunk_copy(h, o).wait_send())
        half_copy(h).wait_send()
        y_copy(h).wait_send()
        loop(1, 4, lambda o: x_copy(h, o).wait_send())
        loop(0, 4, lambda o: core_copy(h, o).wait_send())
        loop(1, 16, lambda o: scale_copy(h, o).wait_send())
        loop(1, 16, lambda o: col_copy(h, o).wait_send())
        return 0

    lax.fori_loop(0, 4, drain, 0)


def per_device(orbitals, potential_slots, pattern_owner, retained, band_energy):
    smem = pl.BlockSpec(memory_space=pltpu.SMEM)
    vmem = pl.BlockSpec(memory_space=pltpu.VMEM)
    dma = pltpu.SemaphoreType.DMA
    out = pl.pallas_call(
        kernel,
        out_shape=pltpu.VMEM((2048, 128), F32),
        in_specs=[smem] * 3 + [vmem] + [pl.BlockSpec(memory_space=pltpu.HBM)] * 2,
        out_specs=vmem,
        scratch_shapes=[
            pltpu.VMEM((2, 8, 128, 128), BF16),
            pltpu.VMEM((2, 8, 128, 128), BF16),
            pltpu.VMEM((2, 256, 256), BF16),
            pltpu.VMEM((128, 256), BF16),
            pltpu.VMEM((256, 128), BF16),
            pltpu.VMEM((8, 64, 128), F32),
            pltpu.VMEM((4, 16, 2, 16, 128), BF16),
            pltpu.VMEM((4, 2, 4, 2, 16, 128), BF16),
            pltpu.VMEM((4, 8, 2, 4, 2, 16, 128), BF16),
            pltpu.VMEM((16 * PAD, 128), F32),
            pltpu.VMEM((4, 16, 8, 8, 128), BF16),
            pltpu.VMEM((4, 16, 8, 8, 128), BF16),
            pltpu.VMEM((4, 1, 128), F32),
            pltpu.VMEM((4, 16, 1, 128), F32),
            pltpu.VMEM((4096, 128), F32),
            pltpu.VMEM((8, 128, 512), F32),
            dma((2,)), dma((4, 16)), dma((4, 16)), dma((4,)), dma((4,)), dma((4,)), dma((4,)),
            dma((4, 4)), dma((4, 4)), dma((4, 4)), dma((4, 4)),
            dma((4, 16)), dma((4, 16)), dma((4, 16)), dma((4, 16)),
        ],
        compiler_params=pltpu.CompilerParams(
            collective_id=0, has_side_effects=True, vmem_limit_bytes=65994752
        ),
    )(
        pattern_owner, band_energy, retained, retained,
        pltpu.with_memory_space_constraint(orbitals, pltpu.HBM),
        pltpu.with_memory_space_constraint(potential_slots, pltpu.HBM),
    )
    return out.reshape(2, 4, 64, 4, 128)


def solution(mesh):
    in_specs = (
        P("band", "plane", None, None),
        P("band", None, "plane", None, None),
        P(),
        P(),
        P("band"),
    )
    out_specs = P("band", None, None, "plane", None)
    return jax.shard_map(
        per_device, mesh=mesh, in_specs=in_specs, out_specs=out_specs, check_vma=False
    )
```

```python
import functools
import math

import jax
import jax.numpy as jnp
from jax import lax
from jax.experimental import pallas as pl
from jax.experimental.pallas import tpu as pltpu
from jax.sharding import PartitionSpec as P

kinetic_coef = 0.5 * (2.0 * math.pi / 64.0) ** 2
MESH = pl.DeviceIdType.MESH
F32 = jnp.float32
BF16 = jnp.bfloat16
PAD = 72
UNR = True
POWER = 17.5
RANGE = 8192.0
SHIFT = 125.0 * math.log(2.0)


def table(phase):
    half = (((phase + 64) & 127) - 64).astype(F32) * (math.pi / 128)
    square = half * half
    series = jnp.full_like(half, 1.0 / math.factorial(13))
    for n in (11, 9, 7, 5, 3, 1):
        series = (1.0 if n % 4 == 1 else -1.0) / math.factorial(n) + series * square
    sine = half * series
    return (1.0 - 2.0 * sine * sine) * (1.0 / math.sqrt(128))


def signed_square(frequency):
    signed = jnp.where(frequency < 64, frequency, frequency - 128).astype(F32)
    return signed * signed


def iota(shape, dimension):
    return lax.broadcasted_iota(jnp.int32, shape, dimension)


def encode(value, inverse_scale):
    u = jnp.abs(value) * inverse_scale
    w = u + jnp.sqrt(u * u + 1.0)
    code = jnp.exp(POWER * jnp.log(w) - SHIFT)
    return jnp.where(value < 0.0, -code, code).astype(BF16)


def decode(code, scale):
    code = code.astype(F32)
    w = jnp.exp((jnp.log(jnp.abs(code)) + SHIFT) * (1.0 / POWER))
    u = (0.5 * scale) * (w - 1.0 / w)
    return jnp.where(code < 0.0, -u, u)


def parts(value):
    high = value.astype(BF16)
    return high, (value - high.astype(F32)).astype(BF16)


def dot(a, b):
    return jnp.dot(a, b, preferred_element_type=F32)


def loop(low, high, step):
    def body(o, _):
        step(o)
        return 0

    lax.fori_loop(low, high, body, 0, unroll=UNR)


def kernel(
    owner, energy, kept_scalar, kept, orb_hbm, slot_hbm, out,
    orb, slot, wz, wy, wx, precond,
    chunks, picked, pot, cols, sent, got, scale_out, scale_in, plain, partial,
    load, a_send, a_recv, b_send, b_recv, y_send, y_recv, x_send, x_recv, c_send, c_recv,
    d_send, d_recv, s_send, s_recv, rounds,
):
    band, plane = lax.axis_index("band"), lax.axis_index("plane")
    row, spot = band // 8, band % 8
    half, upper = row // 2, row % 2
    member = band % 16
    col, core = spot // 2, spot % 2

    def remote(src, dst, send_sem, recv_sem, **to):
        return pltpu.make_async_remote_copy(
            src_ref=src, dst_ref=dst, send_sem=send_sem, recv_sem=recv_sem,
            device_id=to, device_id_type=MESH,
        )

    load_slot = pltpu.make_async_copy(slot_hbm.at[0], slot, load.at[0])
    load_orb = pltpu.make_async_copy(orb_hbm, orb, load.at[1])
    load_slot.start()
    load_orb.start()

    barrier = pltpu.get_barrier_semaphore()

    def greet(semaphore, **to):
        pl.semaphore_signal(semaphore, 1, device_id=to, device_id_type=MESH)

    def greet_along_z(semaphore, distance):
        for step in (distance, 8 - distance):
            greet(semaphore, plane=plane // 8 * 8 + (plane + step) % 8)

    greet(barrier, plane=(plane + 8) % 16)
    loop(1, 16, lambda o: greet(barrier, band=half * 16 + (member + o) % 16))
    greet(barrier, band=(band + 16) % 32)
    greet_along_z(barrier, 1)
    pl.semaphore_wait(barrier, 19)
    greet_along_z(rounds.at[0], 1)
    load_slot.wait()

    def chunk_of(h, to_spot, to_upper):
        rows = pl.multiple_of(to_spot % 4 * 32 + to_upper * 16, 16)
        return slot.at[:, 2 * h + to_spot // 4, pl.ds(rows, 16), :]

    def chunk_copy(h, o):
        peer = (member + o) % 16
        return remote(
            chunk_of(h, peer % 8, peer // 8), chunks.at[h, member],
            a_send.at[h, o], a_recv.at[h, o], band=half * 16 + peer,
        )

    def chunk_arrival(h, o):
        src = (member - o + 16) % 16
        return remote(
            chunks.at[h, src], chunks.at[h, src],
            a_send.at[h, o], a_recv.at[h, o], band=half * 16 + src,
        )

    def half_copy(h):
        return remote(
            picked.at[h, 0], picked.at[h, 1], b_send.at[h], b_recv.at[h], band=(band + 16) % 32
        )

    def half_arrival(h):
        return remote(
            picked.at[h, 1], picked.at[h, 1], b_send.at[h], b_recv.at[h], band=(band + 16) % 32
        )

    def neighbour():
        return half * 16 + (1 - upper) * 8 + spot

    def y_copy(h):
        return remote(
            pot.at[h, spot, upper], pot.at[h, spot, upper],
            y_send.at[h], y_recv.at[h], band=neighbour(),
        )

    def y_arrival(h):
        return remote(
            pot.at[h, spot, 1 - upper], pot.at[h, spot, 1 - upper],
            y_send.at[h], y_recv.at[h], band=neighbour(),
        )

    def x_copy(h, o):
        return remote(
            pot.at[h, spot], pot.at[h, spot], x_send.at[h, o], x_recv.at[h, o],
            band=row * 8 + (col + o) % 4 * 2 + core,
        )

    def x_arrival(h, o):
        src = (col - o + 4) % 4 * 2 + core
        return remote(
            pot.at[h, src], pot.at[h, src], x_send.at[h, o], x_recv.at[h, o], band=row * 8 + src
        )

    def core_copy(h, o):
        src = (col - o + 4) % 4 * 2 + core
        return remote(
            pot.at[h, src], pot.at[h, src], c_send.at[h, o], c_recv.at[h, o],
            band=row * 8 + col * 2 + 1 - core,
        )

    def core_arrival(h, o):
        src = (col - o + 4) % 4 * 2 + 1 - core
        return remote(
            pot.at[h, src], pot.at[h, src], c_send.at[h, o], c_recv.at[h, o],
            band=row * 8 + col * 2 + 1 - core,
        )

    def col_copy(h, o):
        peer = (plane + o) % 16
        return remote(
            sent.at[h, peer], got.at[h, plane], d_send.at[h, o], d_recv.at[h, o], plane=peer
        )

    def col_arrival(h, o):
        src = (plane - o + 16) % 16
        return remote(
            got.at[h, src], got.at[h, src], d_send.at[h, o], d_recv.at[h, o], plane=src
        )

    def scale_copy(h, o):
        return remote(
            scale_out.at[h], scale_in.at[h, plane], s_send.at[h, o], s_recv.at[h, o],
            plane=(plane + o) % 16,
        )

    def scale_arrival(h, o):
        src = (plane - o + 16) % 16
        return remote(
            scale_in.at[h, src], scale_in.at[h, src], s_send.at[h, o], s_recv.at[h, o], plane=src
        )

    def send_chunks(h):
        loop(1, 16, lambda o: chunk_copy(h, o).start())
        rows = pl.multiple_of(spot % 4 * 32 + upper * 16, 16)
        chunks[h, member] = slot[:, 2 * h + spot // 4, pl.ds(rows, 16), :]

    send_chunks(0)
    send_chunks(1)

    lane4 = iota((1, 256), 1) // 64
    shift_top = jnp.where(lane4 == 1, 32, jnp.where(lane4 == 2, 96, 0))
    shift_low = jnp.where(lane4 == 1, 0, jnp.where(lane4 == 2, 64, 96))
    position = iota((256, 256), 0)
    freq_z = jnp.concatenate([kept[2:3, :]] * 4, axis=1)
    phase = (position & 127) * freq_z + jnp.where(position < 128, shift_top, shift_low)
    high, low = parts(table(phase))
    wz[0] = high
    wz[1] = low
    quarter = jnp.where(iota((1, 128), 1) < 64, 0, 32)
    position = iota((128, 128), 0)
    freq_y = jnp.concatenate([kept[1:2, :]] * 2, axis=1)
    cols[0:128, :] = table(position * freq_y + quarter).T
    for j in range(4):
        for k in range(2):
            high, low = parts(cols[pl.ds(k * 64 + j, 16, stride=4), :])
            wy[j * 16 : j * 16 + 16, k * 128 : k * 128 + 128] = high
            wy[64 + j * 16 : 80 + j * 16, k * 128 : k * 128 + 128] = low
    load_orb.wait()

    def pick(h):
        loop(1, 16, lambda o: chunk_arrival(h, o).wait_recv())
        wanted = [owner[p] % 16 for p in range(4)]
        found = [chunks[h, 0]] * 4
        for m in range(1, 16):
            chunk = chunks[h, m]
            found = [jnp.where(wanted[p] == m, chunk, found[p]) for p in range(4)]
        for p in range(4):
            picked[h, 0, p] = found[p]
        half_copy(h).start()

    def settle(h):
        half_arrival(h).wait_recv()
        for p in range(4):
            inside = owner[p] // 16 == half
            pot[h, spot, upper, p] = jnp.where(inside, picked[h, 0, p], picked[h, 1, p])
        y_copy(h).start()

    def spread(h):
        y_arrival(h).wait_recv()
        loop(1, 4, lambda o: x_copy(h, o).start())
        core_copy(h, 0).start()

    def forward(h):
        def step(o):
            x_arrival(h, o).wait_recv()
            core_copy(h, o).start()

        loop(1, 4, step)

    def transform(h):
        loop(0, 4, lambda o: core_arrival(h, o).wait_recv())

        def band_step(b, top):
            products = []
            for p in range(4):
                for k in range(2):
                    orbital = orb[b, 2 * h + k].astype(F32)
                    real = pot[h, k * 4 : k * 4 + 4, :, p, 0].reshape(128, 128).astype(F32)
                    imag = pot[h, k * 4 : k * 4 + 4, :, p, 1].reshape(128, 128).astype(F32)
                    products.append(jnp.concatenate([orbital * real, orbital * imag], axis=1))
            high, low = parts(jnp.concatenate(products, axis=0))
            z = dot(high, wz[0]) + (dot(low, wz[0]) + dot(high, wz[1]))
            for p in range(4):
                even = z[p * 256 : p * 256 + 128]
                odd = z[p * 256 + 128 : p * 256 + 256]
                pair = jnp.concatenate(
                    [
                        jnp.concatenate([even[:, :128], odd[:, :128]], axis=1),
                        jnp.concatenate([even[:, 128:], odd[:, 128:]], axis=1),
                    ],
                    axis=0,
                )
                high, low = parts(pair)
                both = dot(wy[...], high)
                y = both[:64] + (both[64:] + dot(wy[:64], low))
                for k in range(2):
                    for j in range(4):
                        cols[pl.ds(b * 32 + p * 8 + k * 4 + j, 16, stride=PAD), :] = y[
                            j * 16 : j * 16 + 16, k * 128 : k * 128 + 128
                        ]
                top = jnp.maximum(top, jnp.maximum(jnp.abs(y[:, :128]), jnp.abs(y[:, 128:])))
            return top

        top = lax.fori_loop(0, 2, band_step, jnp.zeros((64, 128), F32))
        top = jnp.max(jnp.max(top, axis=0, keepdims=True), axis=1, keepdims=True)
        scale = jnp.maximum(top, 1e-30) * (1.0 / RANGE)
        inverse = 1.0 / scale
        scale_out[h] = jnp.broadcast_to(scale, (1, 128))
        scale_in[h, plane] = jnp.broadcast_to(scale, (1, 128))

        def encode_step(d, _):
            block = cols[pl.ds(pl.multiple_of(d * PAD, 8), 64), :]
            sent[h, d] = encode(block, inverse).reshape(8, 8, 128)
            return 0

        lax.fori_loop(0, 16, encode_step, 0, unroll=4)
        loop(1, 16, lambda o: scale_copy(h, o).start())
        loop(1, 16, lambda o: col_copy(h, o).start())
        got[h, plane] = sent[h, plane]

    for t in range(8):
        if t >= 4:
            transform(t - 4)
        if 3 <= t < 7:
            forward(t - 3)
        if 2 <= t < 6:
            spread(t - 2)
        if 1 <= t < 5:
            settle(t - 1)
        if t < 4:
            pick(t)
        if t < 2:
            send_chunks(t + 2)
        if t < 3:
            pl.semaphore_wait(rounds.at[t], 2)
        if t < 2:
            greet_along_z(rounds.at[t + 1], 2 - t)

    freq_x = jnp.concatenate([kept[0:1, :]] * 2, axis=1)
    position = position // 2 % 16 * 8 + position // 32 * 2 + position % 2
    high, low = parts(table(position * freq_x + quarter).T)
    wx[:128] = high
    wx[128:] = low
    kx2 = jnp.broadcast_to(signed_square(freq_x), (128, 128)).T[:64]
    kz2 = signed_square(jnp.concatenate([kept[2:3, :]] * 2, axis=1))
    for j in range(4):
        ky2 = signed_square(kept_scalar[1, plane * 4 + j])
        kinetic = kinetic_coef * (kx2 + ky2 + kz2)
        for b in range(2):
            precond[b * 4 + j] = 1.0 / (1.0 + kinetic / energy[b])

    def receive(h):
        loop(1, 16, lambda o: scale_arrival(h, o).wait_recv())
        loop(1, 16, lambda o: col_arrival(h, o).wait_recv())
        scales = scale_in[h]
        for n in range(8):
            rows = pl.multiple_of(n * 512 + h * 128, 128)
            plain[pl.ds(rows, 128), :] = decode(got[h, :, n], scales).reshape(128, 128)

    def x_sum(n, first, count):
        blocks = [plain[pl.ds(n * 512 + first * 128 + j, 32 * count, stride=4), :] for j in range(4)]
        high, low = parts(jnp.concatenate(blocks, axis=1))
        keys = slice(first * 32, (first + count) * 32)
        both = dot(wx[:, keys], high)
        return both[:128] + (both[128:] + dot(wx[:128, keys], low))

    lane = iota((64, 128), 1)

    def begin(n, _):
        partial[n] = x_sum(n, 0, 3)
        return 0

    def finish(n, _):
        x = partial[n] + x_sum(n, 3, 1)
        for j in range(4):
            cosine = x[:64, j * 128 : j * 128 + 128]
            sine = pltpu.roll(x[64:, j * 128 : j * 128 + 128], 64, 1)
            value = cosine + jnp.where(lane < 64, -sine, sine)
            out[pl.ds(n * 256 + j, 64, stride=4), :] = value * precond[n // 4 * 4 + j]
        return 0

    for h in range(3):
        receive(h)
    lax.fori_loop(0, 8, begin, 0, unroll=2)
    receive(3)
    lax.fori_loop(0, 8, finish, 0, unroll=2)

    def drain(h, _):
        loop(1, 16, lambda o: chunk_copy(h, o).wait_send())
        half_copy(h).wait_send()
        y_copy(h).wait_send()
        loop(1, 4, lambda o: x_copy(h, o).wait_send())
        loop(0, 4, lambda o: core_copy(h, o).wait_send())
        loop(1, 16, lambda o: scale_copy(h, o).wait_send())
        loop(1, 16, lambda o: col_copy(h, o).wait_send())
        return 0

    lax.fori_loop(0, 4, drain, 0)


def per_device(orbitals, potential_slots, pattern_owner, retained, band_energy):
    smem = pl.BlockSpec(memory_space=pltpu.SMEM)
    vmem = pl.BlockSpec(memory_space=pltpu.VMEM)
    dma = pltpu.SemaphoreType.DMA
    out = pl.pallas_call(
        kernel,
        out_shape=pltpu.VMEM((2048, 128), F32),
        in_specs=[smem] * 3 + [vmem] + [pl.BlockSpec(memory_space=pltpu.HBM)] * 2,
        out_specs=vmem,
        scratch_shapes=[
            pltpu.VMEM((2, 8, 128, 128), BF16),
            pltpu.VMEM((2, 8, 128, 128), BF16),
            pltpu.VMEM((2, 256, 256), BF16),
            pltpu.VMEM((128, 256), BF16),
            pltpu.VMEM((256, 128), BF16),
            pltpu.VMEM((8, 64, 128), F32),
            pltpu.VMEM((4, 16, 2, 16, 128), BF16),
            pltpu.VMEM((4, 2, 4, 2, 16, 128), BF16),
            pltpu.VMEM((4, 8, 2, 4, 2, 16, 128), BF16),
            pltpu.VMEM((16 * PAD, 128), F32),
            pltpu.VMEM((4, 16, 8, 8, 128), BF16),
            pltpu.VMEM((4, 16, 8, 8, 128), BF16),
            pltpu.VMEM((4, 1, 128), F32),
            pltpu.VMEM((4, 16, 1, 128), F32),
            pltpu.VMEM((4096, 128), F32),
            pltpu.VMEM((8, 128, 512), F32),
            dma((2,)), dma((4, 16)), dma((4, 16)), dma((4,)), dma((4,)), dma((4,)), dma((4,)),
            dma((4, 4)), dma((4, 4)), dma((4, 4)), dma((4, 4)),
            dma((4, 16)), dma((4, 16)), dma((4, 16)), dma((4, 16)),
            pltpu.SemaphoreType.REGULAR((3,)),
        ],
        compiler_params=pltpu.CompilerParams(
            collective_id=0, has_side_effects=True, vmem_limit_bytes=65994752
        ),
    )(
        pattern_owner, band_energy, retained, retained,
        pltpu.with_memory_space_constraint(orbitals, pltpu.HBM),
        pltpu.with_memory_space_constraint(potential_slots, pltpu.HBM),
    )
    return out.reshape(2, 4, 64, 4, 128)


def solution(mesh):
    in_specs = (
        P("band", "plane", None, None),
        P("band", None, "plane", None, None),
        P(),
        P(),
        P("band"),
    )
    out_specs = P("band", None, None, "plane", None)
    return jax.shard_map(
        per_device, mesh=mesh, in_specs=in_specs, out_specs=out_specs, check_vma=False
    )
```

```python
import functools
import math

import jax
import jax.numpy as jnp
from jax import lax
from jax.experimental import pallas as pl
from jax.experimental.pallas import tpu as pltpu
from jax.sharding import PartitionSpec as P

kinetic_coef = 0.5 * (2.0 * math.pi / 64.0) ** 2
MESH = pl.DeviceIdType.MESH
F32 = jnp.float32
BF16 = jnp.bfloat16
PAD = 72
UNR = True
POWER = 17.5
RANGE = 8192.0
SHIFT = 125.0 * math.log(2.0)


def table(phase):
    half = (((phase + 64) & 127) - 64).astype(F32) * (math.pi / 128)
    square = half * half
    series = jnp.full_like(half, 1.0 / math.factorial(13))
    for n in (11, 9, 7, 5, 3, 1):
        series = (1.0 if n % 4 == 1 else -1.0) / math.factorial(n) + series * square
    sine = half * series
    return (1.0 - 2.0 * sine * sine) * (1.0 / math.sqrt(128))


def signed_square(frequency):
    signed = jnp.where(frequency < 64, frequency, frequency - 128).astype(F32)
    return signed * signed


def iota(shape, dimension):
    return lax.broadcasted_iota(jnp.int32, shape, dimension)


def encode(value, inverse_scale):
    u = jnp.abs(value) * inverse_scale
    w = u + jnp.sqrt(u * u + 1.0)
    code = jnp.exp(POWER * jnp.log(w) - SHIFT)
    return jnp.where(value < 0.0, -code, code).astype(BF16)


def decode(code, scale):
    code = code.astype(F32)
    w = jnp.exp((jnp.log(jnp.abs(code)) + SHIFT) * (1.0 / POWER))
    u = (0.5 * scale) * (w - 1.0 / w)
    return jnp.where(code < 0.0, -u, u)


def parts(value):
    high = value.astype(BF16)
    return high, (value - high.astype(F32)).astype(BF16)


def dot(a, b):
    return jnp.dot(a, b, preferred_element_type=F32)


def loop(low, high, step):
    def body(o, _):
        step(o)
        return 0

    lax.fori_loop(low, high, body, 0, unroll=UNR)


def kernel(
    owner, energy, kept_scalar, kept, orb_hbm, slot_hbm, out,
    orb, slot, wz, wy, wx, precond,
    chunks, picked, pot, cols, sent, got, scale_out, scale_in, plain, partial,
    load, a_send, a_recv, b_send, b_recv, y_send, y_recv, x_send, x_recv, c_send, c_recv,
    d_send, d_recv, s_send, s_recv, rounds,
):
    band, plane = lax.axis_index("band"), lax.axis_index("plane")
    row, spot = band // 8, band % 8
    half, upper = row // 2, row % 2
    member = band % 16
    col, core = spot // 2, spot % 2

    def remote(src, dst, send_sem, recv_sem, **to):
        return pltpu.make_async_remote_copy(
            src_ref=src, dst_ref=dst, send_sem=send_sem, recv_sem=recv_sem,
            device_id=to, device_id_type=MESH,
        )

    load_slot = pltpu.make_async_copy(slot_hbm.at[0], slot, load.at[0])
    load_orb = pltpu.make_async_copy(orb_hbm, orb, load.at[1])
    load_slot.start()
    load_orb.start()

    barrier = pltpu.get_barrier_semaphore()

    def greet(semaphore, **to):
        pl.semaphore_signal(semaphore, 1, device_id=to, device_id_type=MESH)

    def greet_along_z(semaphore, distance):
        for step in (distance, 8 - distance):
            greet(semaphore, plane=plane // 8 * 8 + (plane + step) % 8)

    greet(barrier, plane=(plane + 8) % 16)
    loop(1, 16, lambda o: greet(barrier, band=half * 16 + (member + o) % 16))
    greet(barrier, band=(band + 16) % 32)
    greet_along_z(barrier, 1)
    pl.semaphore_wait(barrier, 19)
    greet_along_z(rounds.at[0], 1)
    load_slot.wait()

    def chunk_of(h, to_spot, to_upper):
        rows = pl.multiple_of(to_spot % 4 * 32 + to_upper * 16, 16)
        return slot.at[:, 2 * h + to_spot // 4, pl.ds(rows, 16), :]

    def chunk_copy(h, o):
        peer = (member + o) % 16
        return remote(
            chunk_of(h, peer % 8, peer // 8), chunks.at[h, member],
            a_send.at[h, o], a_recv.at[h, o], band=half * 16 + peer,
        )

    def chunk_arrival(h, o):
        src = (member - o + 16) % 16
        return remote(
            chunks.at[h, src], chunks.at[h, src],
            a_send.at[h, o], a_recv.at[h, o], band=half * 16 + src,
        )

    def half_copy(h):
        return remote(
            picked.at[h, 0], picked.at[h, 1], b_send.at[h], b_recv.at[h], band=(band + 16) % 32
        )

    def half_arrival(h):
        return remote(
            picked.at[h, 1], picked.at[h, 1], b_send.at[h], b_recv.at[h], band=(band + 16) % 32
        )

    def neighbour():
        return half * 16 + (1 - upper) * 8 + spot

    def y_copy(h):
        return remote(
            pot.at[h, spot, upper], pot.at[h, spot, upper],
            y_send.at[h], y_recv.at[h], band=neighbour(),
        )

    def y_arrival(h):
        return remote(
            pot.at[h, spot, 1 - upper], pot.at[h, spot, 1 - upper],
            y_send.at[h], y_recv.at[h], band=neighbour(),
        )

    def x_copy(h, o):
        return remote(
            pot.at[h, spot], pot.at[h, spot], x_send.at[h, o], x_recv.at[h, o],
            band=row * 8 + (col + o) % 4 * 2 + core,
        )

    def x_arrival(h, o):
        src = (col - o + 4) % 4 * 2 + core
        return remote(
            pot.at[h, src], pot.at[h, src], x_send.at[h, o], x_recv.at[h, o], band=row * 8 + src
        )

    def core_copy(h, o):
        src = (col - o + 4) % 4 * 2 + core
        return remote(
            pot.at[h, src], pot.at[h, src], c_send.at[h, o], c_recv.at[h, o],
            band=row * 8 + col * 2 + 1 - core,
        )

    def core_arrival(h, o):
        src = (col - o + 4) % 4 * 2 + 1 - core
        return remote(
            pot.at[h, src], pot.at[h, src], c_send.at[h, o], c_recv.at[h, o],
            band=row * 8 + col * 2 + 1 - core,
        )

    def col_copy(h, o):
        peer = (plane + o) % 16
        return remote(
            sent.at[h, peer], got.at[h, plane], d_send.at[h, o], d_recv.at[h, o], plane=peer
        )

    def col_arrival(h, o):
        src = (plane - o + 16) % 16
        return remote(
            got.at[h, src], got.at[h, src], d_send.at[h, o], d_recv.at[h, o], plane=src
        )

    def scale_copy(h, o):
        return remote(
            scale_out.at[h], scale_in.at[h, plane], s_send.at[h, o], s_recv.at[h, o],
            plane=(plane + o) % 16,
        )

    def scale_arrival(h, o):
        src = (plane - o + 16) % 16
        return remote(
            scale_in.at[h, src], scale_in.at[h, src], s_send.at[h, o], s_recv.at[h, o], plane=src
        )

    def send_chunks(h):
        loop(1, 16, lambda o: chunk_copy(h, o).start())
        rows = pl.multiple_of(spot % 4 * 32 + upper * 16, 16)
        chunks[h, member] = slot[:, 2 * h + spot // 4, pl.ds(rows, 16), :]

    send_chunks(0)
    send_chunks(1)

    lane4 = iota((1, 256), 1) // 64
    shift_top = jnp.where(lane4 == 1, 32, jnp.where(lane4 == 2, 96, 0))
    shift_low = jnp.where(lane4 == 1, 0, jnp.where(lane4 == 2, 64, 96))
    position = iota((256, 256), 0)
    freq_z = jnp.concatenate([kept[2:3, :]] * 4, axis=1)
    phase = (position & 127) * freq_z + jnp.where(position < 128, shift_top, shift_low)
    high, low = parts(table(phase))
    wz[0] = high
    wz[1] = low
    quarter = jnp.where(iota((1, 128), 1) < 64, 0, 32)
    position = iota((128, 128), 0)
    freq_y = jnp.concatenate([kept[1:2, :]] * 2, axis=1)
    cols[0:128, :] = table(position * freq_y + quarter).T
    for j in range(4):
        for k in range(2):
            high, low = parts(cols[pl.ds(k * 64 + j, 16, stride=4), :])
            wy[j * 16 : j * 16 + 16, k * 128 : k * 128 + 128] = high
            wy[64 + j * 16 : 80 + j * 16, k * 128 : k * 128 + 128] = low
    load_orb.wait()

    def pick(h):
        loop(1, 16, lambda o: chunk_arrival(h, o).wait_recv())
        wanted = [owner[p] % 16 for p in range(4)]
        found = [chunks[h, 0]] * 4
        for m in range(1, 16):
            chunk = chunks[h, m]
            found = [jnp.where(wanted[p] == m, chunk, found[p]) for p in range(4)]
        for p in range(4):
            picked[h, 0, p] = found[p]
        half_copy(h).start()

    def settle(h):
        half_arrival(h).wait_recv()
        for p in range(4):
            inside = owner[p] // 16 == half
            pot[h, spot, upper, p] = jnp.where(inside, picked[h, 0, p], picked[h, 1, p])
        y_copy(h).start()

    def spread(h):
        y_arrival(h).wait_recv()
        loop(1, 4, lambda o: x_copy(h, o).start())
        core_copy(h, 0).start()

    def forward(h):
        def step(o):
            x_arrival(h, o).wait_recv()
            core_copy(h, o).start()

        loop(1, 4, step)

    def transform(h):
        loop(0, 4, lambda o: core_arrival(h, o).wait_recv())

        def band_step(b, top):
            products = []
            for p in range(4):
                for k in range(2):
                    orbital = orb[b, 2 * h + k].astype(F32)
                    real = pot[h, k * 4 : k * 4 + 4, :, p, 0].reshape(128, 128).astype(F32)
                    imag = pot[h, k * 4 : k * 4 + 4, :, p, 1].reshape(128, 128).astype(F32)
                    products.append(jnp.concatenate([orbital * real, orbital * imag], axis=1))
            high, low = parts(jnp.concatenate(products, axis=0))
            z = dot(high, wz[0]) + (dot(low, wz[0]) + dot(high, wz[1]))
            for p in range(4):
                even = z[p * 256 : p * 256 + 128]
                odd = z[p * 256 + 128 : p * 256 + 256]
                pair = jnp.concatenate(
                    [
                        jnp.concatenate([even[:, :128], odd[:, :128]], axis=1),
                        jnp.concatenate([even[:, 128:], odd[:, 128:]], axis=1),
                    ],
                    axis=0,
                )
                high, low = parts(pair)
                both = dot(wy[...], high)
                y = both[:64] + (both[64:] + dot(wy[:64], low))
                for k in range(2):
                    for j in range(4):
                        cols[pl.ds(b * 32 + p * 8 + k * 4 + j, 16, stride=PAD), :] = y[
                            j * 16 : j * 16 + 16, k * 128 : k * 128 + 128
                        ]
                top = jnp.maximum(top, jnp.maximum(jnp.abs(y[:, :128]), jnp.abs(y[:, 128:])))
            return top

        top = lax.fori_loop(0, 2, band_step, jnp.zeros((64, 128), F32))
        top = jnp.max(jnp.max(top, axis=0, keepdims=True), axis=1, keepdims=True)
        scale = jnp.maximum(top, 1e-30) * (1.0 / RANGE)
        inverse = 1.0 / scale
        scale_out[h] = jnp.broadcast_to(scale, (1, 128))
        scale_in[h, plane] = jnp.broadcast_to(scale, (1, 128))

        def encode_step(d, _):
            block = cols[pl.ds(pl.multiple_of(d * PAD, 8), 64), :]
            sent[h, d] = encode(block, inverse).reshape(8, 8, 128)
            return 0

        lax.fori_loop(0, 16, encode_step, 0, unroll=4)
        loop(1, 16, lambda o: col_copy(h, o).start())
        loop(1, 16, lambda o: scale_copy(h, o).start())
        got[h, plane] = sent[h, plane]

    for t in range(8):
        if t >= 4:
            transform(t - 4)
        if 3 <= t < 7:
            forward(t - 3)
        if 2 <= t < 6:
            spread(t - 2)
        if 1 <= t < 5:
            settle(t - 1)
        if t < 4:
            pick(t)
        if t < 2:
            send_chunks(t + 2)
        if t < 3:
            pl.semaphore_wait(rounds.at[t], 2)
        if t < 2:
            greet_along_z(rounds.at[t + 1], 2 - t)

    freq_x = jnp.concatenate([kept[0:1, :]] * 2, axis=1)
    position = position // 2 % 16 * 8 + position // 32 * 2 + position % 2
    high, low = parts(table(position * freq_x + quarter).T)
    wx[:128] = high
    wx[128:] = low
    kx2 = jnp.broadcast_to(signed_square(freq_x), (128, 128)).T[:64]
    kz2 = signed_square(jnp.concatenate([kept[2:3, :]] * 2, axis=1))
    for j in range(4):
        ky2 = signed_square(kept_scalar[1, plane * 4 + j])
        kinetic = kinetic_coef * (kx2 + ky2 + kz2)
        for b in range(2):
            precond[b * 4 + j] = 1.0 / (1.0 + kinetic / energy[b])

    def receive(h):
        loop(1, 16, lambda o: scale_arrival(h, o).wait_recv())
        loop(1, 16, lambda o: col_arrival(h, o).wait_recv())
        scales = scale_in[h]
        for n in range(8):
            rows = pl.multiple_of(n * 512 + h * 128, 128)
            plain[pl.ds(rows, 128), :] = decode(got[h, :, n], scales).reshape(128, 128)

    def x_sum(n, first, count):
        blocks = [plain[pl.ds(n * 512 + first * 128 + j, 32 * count, stride=4), :] for j in range(4)]
        high, low = parts(jnp.concatenate(blocks, axis=1))
        keys = slice(first * 32, (first + count) * 32)
        both = dot(wx[:, keys], high)
        return both[:128] + (both[128:] + dot(wx[:128, keys], low))

    lane = iota((64, 128), 1)

    def begin(n, _):
        partial[n] = x_sum(n, 0, 3)
        return 0

    def finish(n, _):
        x = partial[n] + x_sum(n, 3, 1)
        for j in range(4):
            cosine = x[:64, j * 128 : j * 128 + 128]
            sine = pltpu.roll(x[64:, j * 128 : j * 128 + 128], 64, 1)
            value = cosine + jnp.where(lane < 64, -sine, sine)
            out[pl.ds(n * 256 + j, 64, stride=4), :] = value * precond[n // 4 * 4 + j]
        return 0

    for h in range(3):
        receive(h)
    lax.fori_loop(0, 8, begin, 0, unroll=2)
    receive(3)
    lax.fori_loop(0, 8, finish, 0, unroll=2)

    def drain(h, _):
        loop(1, 16, lambda o: chunk_copy(h, o).wait_send())
        half_copy(h).wait_send()
        y_copy(h).wait_send()
        loop(1, 4, lambda o: x_copy(h, o).wait_send())
        loop(0, 4, lambda o: core_copy(h, o).wait_send())
        loop(1, 16, lambda o: scale_copy(h, o).wait_send())
        loop(1, 16, lambda o: col_copy(h, o).wait_send())
        return 0

    lax.fori_loop(0, 4, drain, 0)


def per_device(orbitals, potential_slots, pattern_owner, retained, band_energy):
    smem = pl.BlockSpec(memory_space=pltpu.SMEM)
    vmem = pl.BlockSpec(memory_space=pltpu.VMEM)
    dma = pltpu.SemaphoreType.DMA
    out = pl.pallas_call(
        kernel,
        out_shape=pltpu.VMEM((2048, 128), F32),
        in_specs=[smem] * 3 + [vmem] + [pl.BlockSpec(memory_space=pltpu.HBM)] * 2,
        out_specs=vmem,
        scratch_shapes=[
            pltpu.VMEM((2, 8, 128, 128), BF16),
            pltpu.VMEM((2, 8, 128, 128), BF16),
            pltpu.VMEM((2, 256, 256), BF16),
            pltpu.VMEM((128, 256), BF16),
            pltpu.VMEM((256, 128), BF16),
            pltpu.VMEM((8, 64, 128), F32),
            pltpu.VMEM((4, 16, 2, 16, 128), BF16),
            pltpu.VMEM((4, 2, 4, 2, 16, 128), BF16),
            pltpu.VMEM((4, 8, 2, 4, 2, 16, 128), BF16),
            pltpu.VMEM((16 * PAD, 128), F32),
            pltpu.VMEM((4, 16, 8, 8, 128), BF16),
            pltpu.VMEM((4, 16, 8, 8, 128), BF16),
            pltpu.VMEM((4, 1, 128), F32),
            pltpu.VMEM((4, 16, 1, 128), F32),
            pltpu.VMEM((4096, 128), F32),
            pltpu.VMEM((8, 128, 512), F32),
            dma((2,)), dma((4, 16)), dma((4, 16)), dma((4,)), dma((4,)), dma((4,)), dma((4,)),
            dma((4, 4)), dma((4, 4)), dma((4, 4)), dma((4, 4)),
            dma((4, 16)), dma((4, 16)), dma((4, 16)), dma((4, 16)),
            pltpu.SemaphoreType.REGULAR((3,)),
        ],
        compiler_params=pltpu.CompilerParams(
            collective_id=0, has_side_effects=True, vmem_limit_bytes=65994752
        ),
    )(
        pattern_owner, band_energy, retained, retained,
        pltpu.with_memory_space_constraint(orbitals, pltpu.HBM),
        pltpu.with_memory_space_constraint(potential_slots, pltpu.HBM),
    )
    return out.reshape(2, 4, 64, 4, 128)


def solution(mesh):
    in_specs = (
        P("band", "plane", None, None),
        P("band", None, "plane", None, None),
        P(),
        P(),
        P("band"),
    )
    out_specs = P("band", None, None, "plane", None)
    return jax.shard_map(
        per_device, mesh=mesh, in_specs=in_specs, out_specs=out_specs, check_vma=False
    )
```
